32 devices in a mesh: rep: 2 (over core), ep: 16 (over z, y, x).
Axes of the slice: x: 2, y: 2, z: 4, core: 2. Of those that a mesh axis runs over, the one named last changes fastest.
Arguments:
- tokens: bfloat16 [4096, 2048], P(('rep', 'ep')), may hold values from -6 to 6
- gates: float32 [4096], P(('rep', 'ep')), may hold values from 0.25 to 1
- expert_ids: int32 [4096, 1], P(('rep', 'ep')), may hold values from 0 to 3; in each aligned block of 128 rows (0 to 127, 128 to 255, ...) at most 40 rows name the same one
- weight_in: bfloat16 [2048, 16384], P(None, 'ep'), may hold values from -0.125 to 0.125
- weight_out: bfloat16 [16384, 2048], P('ep'), may hold values from -0.09375 to 0.09375
Outputs:
- mixed: bfloat16 [4096, 2048], P(('rep', 'ep'))
The draws below stay inside these ranges and needn't reach their ends.
Inputs may be any that keep to these rules, and one draw needn't show every extreme that they name: `expert_ids`: among the 128 rows of one device no expert is named by more than 40 rows, and some expert is named by exactly that many in some devices' rows; every expert is named somewhere.
All inputs are finite; a program needn't handle non-finite values.
Results may differ from the reference program's by a relative error of at most 0.0057.
Values may be sent and summed in bfloat16 or wider, within the bound.
No kernel may reach another device: no remote copies, remote signals or barrier semaphores. Data moves between devices by JAX's collectives and lax.ppermute only.
A program may use at most 64 MiB of HBM per device.

```python
import math
import jax
import jax.numpy as jnp
import numpy as np
from jax import lax

D = 2048
FF_DEV = 1024
SLICES = 4
FFW = 4096
EXPERTS = 4
TOK_DEV = 128
CAP = 24
OCAP = 16
TOKENS = 4096
DEVICES = 32


def block_scale(key, extent, cuts, smallest, largest):
    factor_of = 1.0
    for position, shards_of in cuts:
        steps = jax.random.uniform(jax.random.fold_in(jax.random.fold_in(key, 6), position), (shards_of,), jnp.float32, smallest / len(cuts), largest / len(cuts))
        factor_of = factor_of * jnp.repeat(jnp.exp(steps), extent[position] // shards_of).reshape((-1,) + (1,) * (len(extent) - 1 - position))
    return factor_of


def assign_block(stream_key, own, number, rows, count, top, bound, slope):
    order = jax.random.permutation(stream_key, count)
    packed, ordinary = portions_of(count, rows * top, bound, slope, True), portions_of(count, rows * top, bound, slope, False)
    places = jnp.arange(count)

    def named(lengths, rotation):
        used = int((lengths > 0).sum())
        fixed = max(1, used // 4)
        shifted = fixed + (places - fixed + rotation * (used - fixed)) % max(1, count - fixed)
        return jnp.zeros((count,), jnp.int32).at[order[jnp.where(places < fixed, places, shifted)]].set(jnp.asarray(lengths, jnp.int32))

    lengths = jnp.where(number % 4 == 0, named(packed, number // 4), named(ordinary, number - number // 4 - 1))
    mixed = jax.random.permutation(jax.random.fold_in(own, 3), count)
    source_of, receiver = mixed[0:count // 2 * 2:2], mixed[1:count // 2 * 2:2]
    slack = jnp.minimum(lengths[source_of] - 1, bound - lengths[receiver]) // 2
    slack = jnp.where((source_of == order[0]) | (receiver == order[0]) | (lengths[receiver] == 0), 0, jnp.maximum(slack, 0))
    shifted = jax.random.randint(jax.random.fold_in(own, 4), (count // 2,), 0, 1 << 20) % (slack + 1)
    lengths = lengths.at[source_of].add(-shifted).at[receiver].add(shifted)
    members = jnp.searchsorted(jnp.cumsum(lengths), jnp.arange(rows * top), side="right").astype(jnp.int32)
    grid = members.reshape(top, rows).T
    grid = grid[jax.random.permutation(jax.random.fold_in(own, 1), rows)]
    rotation = jax.random.randint(jax.random.fold_in(own, 2), (rows, 1), 0, top)
    return jnp.take_along_axis(grid, (jnp.arange(top)[None, :] + rotation) % top, axis=1)


def portions_of(number_of, total, reach, lean, full):
    portions = [(1 << 20) // math.isqrt(standing ** lean) + 1 for standing in range(1, number_of + 1)]
    largest = reach if full else min(reach, max(-(-total // number_of), total * portions[0] // sum(portions)))
    least = 1 if total - largest >= number_of - 1 else 0
    holding, spare = [largest] + [least] * (number_of - 1), total - largest - least * (number_of - 1)
    while spare > 0:
        free = [i for i in range(1, number_of) if holding[i] < largest] or [i for i in range(1, number_of) if holding[i] < reach]
        whole, left = sum([portions[i] for i in free]), spare
        for i in free:
            extra = min(reach - holding[i], max(1, left * portions[i] // whole), spare)
            holding[i] = holding[i] + extra
            spare = spare - extra
    return np.array(holding)


def gaussian(stream_key, extent, deviation, reach, shards=(), kind=jnp.bfloat16):
    level = block_scale(stream_key, extent, shards, -0.22, 0.18) if shards else 1.0
    values = jax.random.normal(stream_key, extent, jnp.float32) * deviation * level
    return jnp.minimum(jnp.maximum(values, -reach), reach).astype(kind)


def setup_inputs(seed: int = 0) -> dict:
    splits = jax.random.split(jax.random.key(seed), 6)
    tokens = gaussian(splits[0], (TOKENS, D), 1.0, 6.0, ((0, 32),))
    gates = jnp.clip(jnp.exp(math.log(1.0) - 1.3862944 * jax.random.uniform(splits[1], (TOKENS,), jnp.float32) ** block_scale(splits[1], (TOKENS,), ((0, 32),), -0.2, 0.2)), 0.25, 1.0)
    expert_ids_keys = jax.random.split(jax.random.fold_in(splits[2], 1), TOKENS // TOK_DEV)
    expert_ids_turns = jax.random.permutation(jax.random.fold_in(splits[2], 3), TOKENS // TOK_DEV)
    expert_ids = jax.vmap(lambda own, number: assign_block(jax.random.fold_in(splits[2], 2), own, number, TOK_DEV, EXPERTS, 1, CAP + OCAP, 2))(expert_ids_keys, expert_ids_turns).reshape((TOKENS, 1))
    weight_in = gaussian(splits[3], (D, EXPERTS * FFW), D ** -0.5, 0.125, ((1, 16),))
    weight_out = gaussian(splits[4], (EXPERTS * FFW, D), FFW ** -0.5, 0.09375, ((0, 16),))
    return {"tokens": tokens, "gates": gates, "expert_ids": expert_ids, "weight_in": weight_in, "weight_out": weight_out}


def reference(tokens, gates, expert_ids, weight_in, weight_out):
    expert_of = expert_ids[:, 0]
    total_rows = tokens.shape[0]
    width = tokens.shape[1]
    block_rows = DEVICES * (CAP + OCAP)
    order = jnp.argsort(expert_of, stable=True).astype(jnp.int32)
    ordered = tokens[order]
    padded = jnp.concatenate([ordered, jnp.zeros((block_rows, width), ordered.dtype)], axis=0)
    counts = jnp.sum((expert_of[:, None] == jnp.arange(EXPERTS, dtype=jnp.int32)[None, :]).astype(jnp.int32), axis=0)
    starts = (jnp.cumsum(counts) - counts).astype(jnp.int32)

    def serve(results, expert):
        start = starts[expert]
        block = lax.dynamic_slice_in_dim(padded, start, block_rows, 0)
        first = lax.dynamic_slice_in_dim(weight_in, expert * FFW, FFW, 1)
        second = lax.dynamic_slice_in_dim(weight_out, expert * FFW, FFW, 0)
        hidden = jnp.maximum(jnp.dot(block, first, preferred_element_type=jnp.float32), 0.0).astype(jnp.bfloat16)
        result = jnp.zeros((block_rows, width), jnp.float32)
        for piece in range(SLICES):
            partial_sum = jnp.dot(hidden[:, piece * FF_DEV:(piece + 1) * FF_DEV], second[piece * FF_DEV:(piece + 1) * FF_DEV, :], preferred_element_type=jnp.float32)
            rounded = lax.optimization_barrier(partial_sum.astype(jnp.bfloat16))
            result = result + rounded.astype(jnp.float32)
        valid = jnp.arange(block_rows, dtype=jnp.int32) < counts[expert]
        previous = lax.dynamic_slice_in_dim(results, start, block_rows, 0)
        merged = jnp.where(valid[:, None], result, previous)
        return lax.dynamic_update_slice_in_dim(results, merged, start, 0), 0

    initial = jnp.zeros((total_rows + block_rows, width), jnp.float32)
    results, unused = lax.scan(serve, initial, jnp.arange(EXPERTS, dtype=jnp.int32))
    expert_out = jnp.zeros((total_rows, width), jnp.float32).at[order].set(results[:total_rows])
    return (gates[:, None] * expert_out).astype(jnp.bfloat16)
```

```python
import functools

import jax
import jax.numpy as jnp
from jax import lax
from jax.experimental import pallas as pl
from jax.experimental.pallas import tpu as pltpu
from jax.sharding import PartitionSpec as P

SLICES = 4
AXES = ("rep", "ep")


def route(partner):
    reps, owners = lax.axis_size("rep"), lax.axis_size("ep")
    pairs = []
    for rep in range(reps):
        for ep in range(owners):
            to_rep, to_ep = partner(rep, ep)
            pairs.append((rep * owners + ep, to_rep * owners + to_ep))
    return pairs


def slots_row(ids_ref, here_ref, experts, seats):
    count = ids_ref.shape[1]
    distance = ids_ref[...] ^ here_ref[0]
    named = (lax.broadcasted_iota(jnp.int32, (experts, count), 0) == distance).astype(jnp.bfloat16)
    earlier = (
        lax.broadcasted_iota(jnp.int32, (count, count), 0)
        < lax.broadcasted_iota(jnp.int32, (count, count), 1)
    ).astype(jnp.bfloat16)
    ahead = jnp.dot(named, earlier, preferred_element_type=jnp.float32)
    rank = jnp.sum(named.astype(jnp.float32) * ahead, axis=0, keepdims=True)
    return distance.astype(jnp.float32) * seats + rank


def pack_kernel(experts, seats, here_ref, ids_ref, tokens_ref, *out_refs):
    count = ids_ref.shape[1]
    slot = slots_row(ids_ref, here_ref, experts, seats).astype(jnp.int32)
    chosen = lax.broadcasted_iota(jnp.int32, (experts * seats, count), 0) == slot
    rows = jnp.dot(
        chosen.astype(jnp.bfloat16), tokens_ref[...], preferred_element_type=jnp.float32
    ).astype(jnp.bfloat16)
    for index, ref in enumerate(out_refs):
        ref[...] = rows[index * seats : (index + 1) * seats]


def unpack_kernel(experts, seats, here_ref, ids_ref, gates_ref, *refs):
    out_ref = refs[-1]
    count = ids_ref.shape[1]
    slot = slots_row(ids_ref, here_ref, experts, seats)
    same = lax.broadcasted_iota(jnp.int32, (count, count), 0) == lax.broadcasted_iota(
        jnp.int32, (count, count), 1
    )
    slot = jnp.sum(jnp.where(same, slot, 0.0), axis=1, keepdims=True).astype(jnp.int32)
    gate = jnp.sum(jnp.where(same, gates_ref[...], 0.0), axis=1, keepdims=True)
    lane = lax.broadcasted_iota(jnp.int32, (count, seats), 1)
    total = jnp.zeros(out_ref.shape, jnp.float32)
    for index, ref in enumerate(refs[:-1]):
        chosen = (slot - index * seats == lane).astype(jnp.bfloat16)
        total = total + jnp.dot(chosen, ref[...], preferred_element_type=jnp.float32)
    out_ref[...] = (total * gate).astype(jnp.bfloat16)


def feed_kernel(rows_ref, weight_in_ref, weight_out_ref, out_ref, hidden_ref):
    inner = weight_in_ref.shape[1]
    width = weight_out_ref.shape[1]
    block = 256

    def first(step, carry):
        columns = pl.ds(pl.multiple_of(step * block, block), block)
        hidden = jnp.dot(
            rows_ref[...], weight_in_ref[:, columns], preferred_element_type=jnp.float32
        )
        hidden_ref[:, columns] = jnp.maximum(hidden, 0.0).astype(jnp.bfloat16)
        return carry

    lax.fori_loop(0, inner // block, first, 0)

    def second(step, carry):
        columns = pl.ds(pl.multiple_of(step * block, block), block)
        out_ref[:, columns] = jnp.dot(
            hidden_ref[...], weight_out_ref[:, columns], preferred_element_type=jnp.float32
        ).astype(jnp.bfloat16)
        return carry

    lax.fori_loop(0, width // block, second, 0)


def feed(rows, weight_in, weight_out):
    count, width = rows.shape
    inner = weight_in.shape[1]
    vmem = pl.BlockSpec(memory_space=pltpu.VMEM)
    return pl.pallas_call(
        feed_kernel,
        out_shape=jax.ShapeDtypeStruct((count, width), jnp.bfloat16),
        in_specs=[vmem] * 3,
        out_specs=vmem,
        scratch_shapes=[pltpu.VMEM((count, inner), jnp.bfloat16)],
        compiler_params=pltpu.CompilerParams(vmem_limit_bytes=24 * 2**20),
        cost_estimate=pl.CostEstimate(
            flops=4 * count * width * inner, bytes_accessed=4 * width * inner, transcendentals=0
        ),
    )(rows, weight_in, weight_out)


def chunks_of(experts):
    if experts == 4:
        return ((0, 1), (3,), (2,))
    half = experts // 2
    return (tuple(range(half)), tuple(range(half, experts)))


def body(tokens, gates, expert_ids, weight_in, weight_out):
    owner_count = lax.axis_size("ep")
    experts = owner_count // SLICES
    tok_rows, width = tokens.shape
    bound = 3 * tok_rows // (4 * experts) + tok_rows // (2 * experts)
    seats = -(-bound // 8) * 8
    here = (lax.axis_index("ep") // SLICES).astype(jnp.int32).reshape(1)
    ids = expert_ids.reshape(1, tok_rows)
    smem = pl.BlockSpec(memory_space=pltpu.SMEM)
    vmem = pl.BlockSpec(memory_space=pltpu.VMEM)

    near = route(lambda rep, ep: (rep, ep ^ (1 if rep % 2 == 0 else 2)))
    far = route(lambda rep, ep: (rep, ep ^ (2 if rep % 2 == 0 else 1)))

    def across(block, distance):
        if distance == 0:
            return block
        return lax.ppermute(block, AXES, route(lambda rep, ep: (rep, ep ^ (SLICES * distance))))

    packed = pl.pallas_call(
        functools.partial(pack_kernel, experts, seats),
        out_shape=[jax.ShapeDtypeStruct((seats, width), jnp.bfloat16)] * experts,
        in_specs=[smem, vmem, vmem],
        out_specs=[vmem] * experts,
    )(here, ids, tokens)

    groups = chunks_of(experts)
    done = [None] * experts
    for group in groups:
        parts = [across(packed[distance], distance) for distance in group]
        mine = parts[0] if len(parts) == 1 else jnp.concatenate(parts, axis=0)
        count = mine.shape[0]
        pair = jnp.concatenate([mine, lax.ppermute(mine, AXES, near)], axis=0)
        other = lax.ppermute(pair, AXES, far)
        give = feed(other, weight_in, weight_out)
        keep = feed(pair, weight_in, weight_out)
        taken = lax.ppermute(give, AXES, far)
        both = keep.astype(jnp.float32) + taken.astype(jnp.float32)
        landed = lax.ppermute(both[count:].astype(jnp.bfloat16), AXES, near)
        total = (both[:count] + landed.astype(jnp.float32)).astype(jnp.bfloat16)
        for index, distance in enumerate(group):
            done[distance] = across(total[index * seats : (index + 1) * seats], distance)

    return pl.pallas_call(
        functools.partial(unpack_kernel, experts, seats),
        out_shape=jax.ShapeDtypeStruct((tok_rows, width), jnp.bfloat16),
        in_specs=[smem] + [vmem] * (experts + 2),
        out_specs=vmem,
    )(here, ids, gates.reshape(1, tok_rows), *done)


def solution(mesh):
    in_specs = (
        P(("rep", "ep"), None),
        P(("rep", "ep")),
        P(("rep", "ep"), None),
        P(None, "ep"),
        P("ep", None),
    )
    out_specs = P(("rep", "ep"), None)
    return jax.shard_map(body, mesh=mesh, in_specs=in_specs, out_specs=out_specs, check_vma=False)
```
